128 devices in a mesh: expert: 16 (over y, x_hi, core), replica: 8 (over z, x_lo).
Axes of the slice: x: 4 (x_hi: 2, x_lo: 2; x = x_hi * 2 + x_lo), y: 4, z: 4, core: 2. Of those that a mesh axis runs over, the one named last changes fastest.
Arguments:
- tokens_in: bfloat16 [32768, 2048], P(('expert', 'replica')), may hold values from -6 to 6
- cotangents: bfloat16 [32768, 8192], P(('expert', 'replica')), may hold values from -0.1796875 to 0.1796875
- left_root: bfloat16 [16, 2048, 2048], P('expert'), may hold values from -2 to 6, as said below
- right_root: bfloat16 [16, 8, 1024, 1024], P('expert', 'replica'), may hold values from -2 to 6, as said below
Outputs:
- update: bfloat16 [16, 2048, 8192], P('expert', None, 'replica')
The draws below stay inside these ranges and needn't reach their ends.
Inputs may be any that keep to these rules, and one draw needn't show every extreme that they name: `left_root`: each matrix is symmetric. `right_root`: each block is symmetric.
All inputs are finite; a program needn't handle non-finite values.
Results may differ from the reference program's by a relative error of at most 0.0058.
Values may be sent and summed in bfloat16 or wider, within the bound.
No kernel may reach another device: no remote copies, remote signals or barrier semaphores. Data moves between devices by JAX's collectives and lax.ppermute only.
A program may use at most 192 MiB of HBM per device.

```python
import math
import jax
import jax.numpy as jnp
from jax import lax

D = 2048
FF = 8192
BLOCK = 1024
EXPERTS = 16
SLOTS = 16
TOKENS = 32768
BLOCKS = 8


def factor_draw(key, leading, order):
    diag_key, noise_key = jax.random.split(key)
    diagonal = jnp.exp(jax.random.uniform(diag_key, leading + (order,), jnp.float32, 0.0, math.log(3.0)))
    random_part = jnp.clip(jax.random.normal(noise_key, leading + (order, order), jnp.float32), -4.0, 4.0)
    random_part = random_part * (0.8 / math.sqrt(order))
    symmetric = 0.5 * (random_part + jnp.swapaxes(random_part, -1, -2))
    identity = jnp.eye(order, dtype=jnp.float32)
    return (symmetric + identity * diagonal[..., None]).astype(jnp.bfloat16)


def draw_left_root(key, part):
    return factor_draw(jax.random.fold_in(key, 11), (EXPERTS,), D)


def draw_right_root(key, part):
    return factor_draw(jax.random.fold_in(key, 12), (EXPERTS, BLOCKS), BLOCK)


def block_scale(rng, dims, cuts, smallest, top_value):
    loudness = 1.0
    for position, shards_of in cuts:
        steps = jax.random.uniform(jax.random.fold_in(jax.random.fold_in(rng, 6), position), (shards_of,), jnp.float32, smallest / len(cuts), top_value / len(cuts))
        loudness = loudness * jnp.repeat(jnp.exp(steps), dims[position] // shards_of).reshape((-1,) + (1,) * (len(dims) - 1 - position))
    return loudness


def centred(stream_key, dims, spread, most, shards=(), kind=jnp.bfloat16):
    values = jax.random.normal(stream_key, dims, jnp.float32) * spread
    if len(shards) > 0:
        values = block_scale(stream_key, dims, shards, -0.22, 0.18) * values
    return jnp.clip(values, min=-most, max=most).astype(kind)


def setup_inputs(seed: int = 0) -> dict:
    streams_of = jax.random.split(jax.random.key(seed), 5)
    return {
        "tokens_in": centred(streams_of[0], (TOKENS, D), 1.0, 6.0, ((0, 128),)),
        "cotangents": centred(streams_of[1], (TOKENS, FF), 0.03, 0.1796875, ((0, 128),)),
        "left_root": draw_left_root(jax.random.fold_in(streams_of[4], 71), 0),
        "right_root": draw_right_root(jax.random.fold_in(streams_of[4], 71), 0),
    }


def per_expert(inputs):
    expert_tokens, expert_cotangents, left_factor, right_factor = inputs
    gradient = jnp.dot(expert_tokens.T, expert_cotangents, preferred_element_type=jnp.float32).astype(jnp.bfloat16)
    blocks = gradient.reshape(D, BLOCKS, BLOCK).astype(jnp.float32)
    applied = jnp.einsum("dbk,bkj->dbj", blocks, right_factor.astype(jnp.float32))
    applied = applied.astype(jnp.bfloat16).reshape(D, FF)
    return jnp.dot(left_factor, applied, preferred_element_type=jnp.float32).astype(jnp.bfloat16)


def reference(tokens_in, cotangents, left_root, right_root):
    token_groups = jnp.moveaxis(tokens_in.reshape(-1, EXPERTS, SLOTS, D), 1, 0).reshape(EXPERTS, -1, D)
    cotangent_groups = jnp.moveaxis(cotangents.reshape(-1, EXPERTS, SLOTS, FF), 1, 0).reshape(EXPERTS, -1, FF)
    return lax.map(per_expert, (token_groups, cotangent_groups, left_root, right_root))
```

```python
import jax
import jax.numpy as jnp
from jax import lax
from jax.experimental import pallas as pl
from jax.experimental.pallas import tpu as pltpu
from jax.sharding import Mesh
from jax.sharding import PartitionSpec as P

EXPERT = ("y", "xh", "c")
REPLICA = ("z", "xl")
PLANE = ("xl", "y", "xh", "c")
BF16 = jnp.bfloat16
F32 = jnp.float32


def shift(value, axis, step):
    size = lax.axis_size(axis)
    return lax.ppermute(value, axis, [(i, (i + step) % size) for i in range(size)])


def columns_of(cotangents, index, groups, width):
    rows = cotangents.shape[0]

    def kernel(index_ref, source, target):
        target[0] = source[...]

    return pl.pallas_call(
        kernel,
        grid_spec=pltpu.PrefetchScalarGridSpec(
            num_scalar_prefetch=1,
            grid=(groups, 2),
            in_specs=[pl.BlockSpec((rows // 2, width), lambda g, h, index: (h, index[0] * groups + g))],
            out_specs=pl.BlockSpec((1, rows // 2, width), lambda g, h, index: (g, h, 0)),
        ),
        out_shape=jax.ShapeDtypeStruct((groups, rows, width), cotangents.dtype),
        name="columns_of",
    )(index.reshape(1), cotangents)


def left_applied(left, tokens):
    halves = 2
    order, count = left.shape[0], tokens.shape[0]
    tile = 256
    steps = order // halves // tile

    def kernel(left_ref, tokens_ref, low_ref, high_ref):
        value = lax.dot_general(
            left_ref[...], tokens_ref[...], (((1,), (1,)), ((), ())), preferred_element_type=F32
        ).astype(BF16)

        @pl.when(pl.program_id(0) < steps)
        def _():
            low_ref[...] = value

        @pl.when(pl.program_id(0) >= steps)
        def _():
            high_ref[...] = value

    return pl.pallas_call(
        kernel,
        grid=(2 * steps,),
        in_specs=[
            pl.BlockSpec((tile, order), lambda i: (i, 0)),
            pl.BlockSpec((count, order), lambda i: (0, 0)),
        ],
        out_specs=[
            pl.BlockSpec((tile, count), lambda i: (jnp.minimum(i, steps - 1), 0)),
            pl.BlockSpec((tile, count), lambda i: (jnp.maximum(i - steps, 0), 0)),
        ],
        out_shape=[jax.ShapeDtypeStruct((order // halves, count), BF16)] * halves,
        compiler_params=pltpu.CompilerParams(dimension_semantics=("arbitrary",)),
        name="left_applied",
    )(left, tokens)


def combined(side, lows, highs, own, rest):
    half, count = lows[0].shape
    width = own.shape[-1]
    tile = 256
    steps = half // tile
    pieces = len(lows)

    def kernel(side_ref, *refs):
        low_refs, high_refs = refs[:pieces], refs[pieces : 2 * pieces]
        right_refs = refs[2 * pieces : 3 * pieces]
        out_ref = refs[-1]
        is_low = pl.program_id(0) < steps

        def run(left_refs):
            total = None
            for left_ref, right_ref in zip(left_refs, right_refs):
                part = jnp.dot(left_ref[...], right_ref[...].reshape(count, width), preferred_element_type=F32)
                total = part if total is None else total + part
            out_ref[...] = total.astype(BF16)

        @pl.when(is_low)
        def _():
            run(low_refs)

        @pl.when(jnp.logical_not(is_low))
        def _():
            run(high_refs)

    sources, slots = rest.shape[1], rest.shape[3]
    low_spec = pl.BlockSpec((tile, count), lambda i, side: (jnp.minimum(i, steps - 1), 0))
    high_spec = pl.BlockSpec((tile, count), lambda i, side: (jnp.maximum(i - steps, 0), 0))
    right_specs, rights = [], []
    for other in (0, 1):
        right_specs.append(pl.BlockSpec((1, count, width), lambda i, side, o=other: ((side[0] + o) % 2, 0, 0)))
        rights.append(own)
        for k in range(rest.shape[2]):
            right_specs.append(
                pl.BlockSpec(
                    (1, sources, 1, slots, width), lambda i, side, o=other, k=k: ((side[0] + o) % 2, 0, k, 0, 0)
                )
            )
            rights.append(rest)
    return pl.pallas_call(
        kernel,
        grid_spec=pltpu.PrefetchScalarGridSpec(
            num_scalar_prefetch=1,
            grid=(2 * steps,),
            in_specs=[low_spec] * pieces + [high_spec] * pieces + right_specs,
            out_specs=pl.BlockSpec((tile, width), lambda i, side: (i, 0)),
        ),
        out_shape=jax.ShapeDtypeStruct((2 * half, width), BF16),
        compiler_params=pltpu.CompilerParams(dimension_semantics=("arbitrary",)),
        name="combined",
    )(side.reshape(1), *lows, *highs, *rights)


def body(tokens_in, cotangents, left_root, right_root):
    left, right = left_root[0], right_root[0, 0]
    width = right.shape[0]
    order = left.shape[0]
    experts = lax.axis_size(EXPERT)
    plane = lax.axis_size(PLANE)
    slots = tokens_in.shape[0] // experts
    z, z_size = lax.axis_index("z"), lax.axis_size("z")
    side, sides = lax.axis_index("xl"), lax.axis_size("xl")

    by_z = [columns_of(cotangents, (z + k) % z_size, sides, width) for k in (2, 1, 3, 0)]
    by_z = [v.reshape(plane, slots, width) for v in by_z]
    far, up, down = shift(by_z[0], "z", 2), shift(by_z[1], "z", 1), shift(by_z[2], "z", -1)

    tokens = tokens_in.reshape(experts, slots, order)
    tokens = lax.all_to_all(tokens, EXPERT, split_axis=0, concat_axis=0, tiled=True)
    low, high = left_applied(left, tokens.reshape(experts * slots, order))
    low_other, high_other = shift(low, "xl", 1), shift(high, "xl", 1)

    own = lax.all_to_all(by_z[3], PLANE, split_axis=0, concat_axis=0, tiled=True)

    lows, highs = [], []
    for a, b in ((low, high), (low_other, high_other)):
        a_up, b_down = shift(a, "z", 1), shift(b, "z", -1)
        a_down, b_up = shift(a, "z", -1), shift(b, "z", 1)
        a_far, b_far = shift(a_up, "z", 1), shift(b_down, "z", -1)
        lows += [a, a_up, a_down, a_far]
        highs += [b, b_up, b_down, b_far]

    rest = jnp.stack([up, down, far], axis=1)
    rest = lax.all_to_all(rest, PLANE, split_axis=0, concat_axis=0, tiled=True)

    own = jnp.dot(own.reshape(-1, width), right, preferred_element_type=F32).astype(BF16)
    rest = jnp.dot(rest.reshape(-1, width), right, preferred_element_type=F32).astype(BF16)
    own = own.reshape(sides, experts * slots, width)
    rest = rest.reshape(sides, experts, z_size - 1, slots, width)
    return combined(side, lows, highs, own, rest)[None]


def solution(mesh):
    split = Mesh(mesh.devices.reshape(4, 2, 2, 4, 2), EXPERT + REPLICA)
    rows = P(EXPERT + REPLICA, None)
    placed = (rows, rows, P(EXPERT, None, None), P(EXPERT, REPLICA, None, None))
    return jax.shard_map(body, mesh=split, in_specs=placed, out_specs=P(EXPERT, None, REPLICA), check_vma=False)
```

```python
import jax
import jax.numpy as jnp
from jax import lax
from jax.experimental import pallas as pl
from jax.experimental.pallas import tpu as pltpu
from jax.sharding import Mesh
from jax.sharding import PartitionSpec as P

EXPERT = ("y", "xh", "c")
REPLICA = ("z", "xl")
PLANE = ("xl", "y", "xh", "c")
BF16 = jnp.bfloat16
F32 = jnp.float32


def shift(value, axis, step):
    size = lax.axis_size(axis)
    return lax.ppermute(value, axis, [(i, (i + step) % size) for i in range(size)])


def exchange(value, axes):
    return lax.all_to_all(value, axes, split_axis=0, concat_axis=0, tiled=True)


def packed(cotangents, steps, groups, width):
    rows = cotangents.shape[0]
    z_size = lax.axis_size("z")

    def kernel(source, *refs):
        targets, semaphore = refs[:-1], refs[-1]
        z = lax.axis_index("z")
        copies = []
        for target, step in zip(targets, steps):
            first = ((z + step) % z_size) * (groups * width)
            for g in range(groups):
                copies.append(
                    pltpu.make_async_copy(
                        source.at[:, pl.ds(pl.multiple_of(first + g * width, width), width)],
                        target.at[g],
                        semaphore.at[len(copies)],
                    )
                )
        for copy in copies:
            copy.start()
        for copy in copies:
            copy.wait()

    return pl.pallas_call(
        kernel,
        in_specs=[pl.BlockSpec(memory_space=pl.ANY)],
        out_specs=[pl.BlockSpec(memory_space=pl.ANY)] * len(steps),
        out_shape=[jax.ShapeDtypeStruct((groups, rows, width), cotangents.dtype)] * len(steps),
        scratch_shapes=[pltpu.SemaphoreType.DMA((len(steps) * groups,))],
        name="packed",
    )(cotangents)


def left_applied(left, tokens):
    order, count = left.shape[0], tokens.shape[0]
    half = order // 2

    def kernel(left_ref, tokens_ref, low_ref, high_ref):
        value = lax.dot_general(
            left_ref[...], tokens_ref[...], (((1,), (1,)), ((), ())), preferred_element_type=F32
        ).astype(BF16)

        @pl.when(pl.program_id(0) == 0)
        def _():
            low_ref[...] = value

        @pl.when(pl.program_id(0) == 1)
        def _():
            high_ref[...] = value

    return pl.pallas_call(
        kernel,
        grid=(2,),
        in_specs=[
            pl.BlockSpec((half, order), lambda i: (i, 0)),
            pl.BlockSpec((count, order), lambda i: (0, 0)),
        ],
        out_specs=[pl.BlockSpec((half, count), lambda i: (0, 0))] * 2,
        out_shape=[jax.ShapeDtypeStruct((half, count), BF16)] * 2,
        compiler_params=pltpu.CompilerParams(dimension_semantics=("arbitrary",)),
        name="left_applied",
    )(left, tokens)


def combined(side, lows, highs, rights, base, out_type):
    half, count = lows[0].shape
    width = rights[0][0].shape[-1]
    tile = 256
    steps = half // tile
    pieces = len(lows)

    def kernel(side_ref, *refs):
        low_refs, high_refs = refs[:pieces], refs[pieces : 2 * pieces]
        right_refs = refs[2 * pieces : 3 * pieces]
        out_ref = refs[-1]
        is_low = pl.program_id(0) < steps

        def run(left_refs):
            left = jnp.concatenate([r[...] for r in left_refs], axis=1)
            right = jnp.concatenate([r[...].reshape(count, width) for r in right_refs], axis=0)
            total = jnp.dot(left, right, preferred_element_type=F32)
            if base is not None:
                total = total + refs[3 * pieces][...]
            out_ref[...] = total.astype(out_type)

        @pl.when(is_low)
        def _():
            run(low_refs)

        @pl.when(jnp.logical_not(is_low))
        def _():
            run(high_refs)

    low_spec = pl.BlockSpec((tile, count), lambda i, side: (jnp.minimum(i, steps - 1), 0))
    high_spec = pl.BlockSpec((tile, count), lambda i, side: (jnp.maximum(i - steps, 0), 0))
    row_spec = pl.BlockSpec((tile, width), lambda i, side: (i, 0))
    right_specs = []
    for value, other, k in rights:
        if k is None:
            right_specs.append(pl.BlockSpec((1, count, width), lambda i, side, o=other: ((side[0] + o) % 2, 0, 0)))
        else:
            block = (1, value.shape[1], 1, value.shape[3], width)
            right_specs.append(pl.BlockSpec(block, lambda i, side, o=other, k=k: ((side[0] + o) % 2, 0, k, 0, 0)))
    bases = [] if base is None else [base]
    return pl.pallas_call(
        kernel,
        grid_spec=pltpu.PrefetchScalarGridSpec(
            num_scalar_prefetch=1,
            grid=(2 * steps,),
            in_specs=[low_spec] * pieces + [high_spec] * pieces + right_specs + [row_spec] * len(bases),
            out_specs=row_spec,
        ),
        out_shape=jax.ShapeDtypeStruct((2 * half, width), out_type),
        compiler_params=pltpu.CompilerParams(dimension_semantics=("arbitrary",)),
        name="combined",
    )(side.reshape(1), *lows, *highs, *[r[0] for r in rights], *bases)


def body(tokens_in, cotangents, left_root, right_root):
    left, right = left_root[0], right_root[0, 0]
    width = right.shape[0]
    order = left.shape[0]
    experts = lax.axis_size(EXPERT)
    plane = lax.axis_size(PLANE)
    slots = tokens_in.shape[0] // experts
    z_size = lax.axis_size("z")
    side, sides = lax.axis_index("xl"), lax.axis_size("xl")

    sent = packed(cotangents, (2, 1, 3), sides, width)
    sent = [v.reshape(plane, slots, width) for v in sent]
    far, up, down = shift(sent[0], "z", 2), shift(sent[1], "z", 1), shift(sent[2], "z", -1)
    kept = packed(cotangents, (0,), sides, width)[0].reshape(plane, slots, width)

    tokens = exchange(tokens_in.reshape(experts, slots, order), EXPERT)
    low, high = left_applied(left, tokens.reshape(experts * slots, order))
    low_other, high_other = shift(low, "xl", 1), shift(high, "xl", 1)

    own = exchange(kept, PLANE)
    rest = exchange(jnp.stack([up, down, far], axis=1), PLANE)

    lows, highs = [], []
    for a, b in ((low, high), (low_other, high_other)):
        a_up, b_down = shift(a, "z", 1), shift(b, "z", -1)
        a_down, b_up = shift(a, "z", -1), shift(b, "z", 1)
        a_far, b_far = shift(a_up, "z", 1), shift(b_down, "z", -1)
        lows.append((a, a_up, a_down, a_far))
        highs.append((b, b_up, b_down, b_far))

    own = jnp.dot(own.reshape(-1, width), right, preferred_element_type=F32).astype(BF16)
    rest = jnp.dot(rest.reshape(-1, width), right, preferred_element_type=F32).astype(BF16)
    own = own.reshape(sides, experts * slots, width)
    rest = rest.reshape(sides, experts, z_size - 1, slots, width)
    most = combined(
        side,
        [v for row in lows for v in row[:3]],
        [v for row in highs for v in row[:3]],
        [r for o in (0, 1) for r in ((own, o, None), (rest, o, 0), (rest, o, 1))],
        None,
        F32,
    )
    update = combined(
        side, [row[3] for row in lows], [row[3] for row in highs], [(rest, 0, 2), (rest, 1, 2)], most, BF16
    )
    return update[None]


def solution(mesh):
    split = Mesh(mesh.devices.reshape(4, 2, 2, 4, 2), EXPERT + REPLICA)
    rows = P(EXPERT + REPLICA, None)
    placed = (rows, rows, P(EXPERT, None, None), P(EXPERT, REPLICA, None, None))

    return jax.shard_map(body, mesh=split, in_specs=placed, out_specs=P(EXPERT, None, REPLICA), check_vma=False)
```

```python
import jax
import jax.numpy as jnp
from jax import lax
from jax.experimental import pallas as pl
from jax.experimental.pallas import tpu as pltpu
from jax.sharding import Mesh
from jax.sharding import PartitionSpec as P

EXPERT = ("y", "xh", "c")
REPLICA = ("z", "xl")
PLANE = ("xl", "y", "xh", "c")
BF16 = jnp.bfloat16
F32 = jnp.float32


def shift(value, axis, step):
    size = lax.axis_size(axis)
    return lax.ppermute(value, axis, [(i, (i + step) % size) for i in range(size)])


def exchange(value, axes):
    return lax.all_to_all(value, axes, split_axis=0, concat_axis=0, tiled=True)


def packed(cotangents, steps, groups, width):
    rows = cotangents.shape[0]
    z_size = lax.axis_size("z")
    pieces = len(steps) * groups

    def kernel(source, *refs):
        targets, (space, arrived, left) = refs[:-3], refs[-3:]
        z = lax.axis_index("z")
        loads, stores = [], []
        for k in range(pieces):
            first = (((z + steps[k // groups]) % z_size) * groups + k % groups) * width
            columns = pl.ds(pl.multiple_of(first, width), width)
            loads.append(pltpu.make_async_copy(source.at[:, columns], space.at[k], arrived.at[k]))
            stores.append(pltpu.make_async_copy(space.at[k], targets[k // groups].at[k % groups], left.at[k]))
        for load in loads:
            load.start()
        for load, store in zip(loads, stores):
            load.wait()
            store.start()
        for store in stores:
            store.wait()

    return pl.pallas_call(
        kernel,
        in_specs=[pl.BlockSpec(memory_space=pltpu.HBM)],
        out_specs=[pl.BlockSpec(memory_space=pltpu.HBM)] * len(steps),
        out_shape=[pltpu.HBM((groups, rows, width), cotangents.dtype)] * len(steps),
        scratch_shapes=[
            pltpu.VMEM((pieces, rows, width), cotangents.dtype),
            pltpu.SemaphoreType.DMA((pieces,)),
            pltpu.SemaphoreType.DMA((pieces,)),
        ],
        compiler_params=pltpu.CompilerParams(vmem_limit_bytes=8 << 20),
        name="packed",
    )(pltpu.with_memory_space_constraint(cotangents, pltpu.HBM))


def left_applied(left, tokens):
    order, count = left.shape[0], tokens.shape[0]
    half = order // 2
    tile = 512
    steps = half // tile

    def kernel(left_ref, tokens_ref, low_ref, high_ref):
        value = lax.dot_general(
            left_ref[...], tokens_ref[...], (((1,), (1,)), ((), ())), preferred_element_type=F32
        ).astype(BF16)

        @pl.when(pl.program_id(0) < steps)
        def _():
            low_ref[...] = value

        @pl.when(pl.program_id(0) >= steps)
        def _():
            high_ref[...] = value

    return pl.pallas_call(
        kernel,
        grid=(2 * steps,),
        in_specs=[
            pl.BlockSpec((tile, order), lambda i: (i, 0)),
            pl.BlockSpec((count, order), lambda i: (0, 0)),
        ],
        out_specs=[
            pl.BlockSpec((tile, count), lambda i: (jnp.minimum(i, steps - 1), 0)),
            pl.BlockSpec((tile, count), lambda i: (jnp.maximum(i - steps, 0), 0)),
        ],
        out_shape=[jax.ShapeDtypeStruct((half, count), BF16)] * 2,
        compiler_params=pltpu.CompilerParams(dimension_semantics=("arbitrary",), vmem_limit_bytes=16 << 20),
        name="left_applied",
    )(left, tokens)


def combined(side, lows, highs, rights, base, out_type):
    half, count = lows[0].shape
    width = rights[0][0].shape[-1]
    tile = 512
    steps = half // tile
    pieces = len(lows)

    def kernel(side_ref, *refs):
        low_refs, high_refs = refs[:pieces], refs[pieces : 2 * pieces]
        right_refs = refs[2 * pieces : 3 * pieces]
        out_ref = refs[-1]
        is_low = pl.program_id(0) < steps

        def run(left_refs):
            left = jnp.concatenate([r[...] for r in left_refs], axis=1)
            right = jnp.concatenate([r[...].reshape(count, width) for r in right_refs], axis=0)
            total = jnp.dot(left, right, preferred_element_type=F32)
            if base is not None:
                total = total + refs[3 * pieces][...]
            out_ref[...] = total.astype(out_type)

        @pl.when(is_low)
        def _():
            run(low_refs)

        @pl.when(jnp.logical_not(is_low))
        def _():
            run(high_refs)

    low_spec = pl.BlockSpec((tile, count), lambda i, side: (jnp.minimum(i, steps - 1), 0))
    high_spec = pl.BlockSpec((tile, count), lambda i, side: (jnp.maximum(i - steps, 0), 0))
    row_spec = pl.BlockSpec((tile, width), lambda i, side: (i, 0))
    right_specs = []
    for value, other, k in rights:
        if k is None:
            right_specs.append(pl.BlockSpec((1, count, width), lambda i, side, o=other: ((side[0] + o) % 2, 0, 0)))
        else:
            block = (1, value.shape[1], 1, value.shape[3], width)
            right_specs.append(pl.BlockSpec(block, lambda i, side, o=other, k=k: ((side[0] + o) % 2, 0, k, 0, 0)))
    bases = [] if base is None else [base]
    return pl.pallas_call(
        kernel,
        grid_spec=pltpu.PrefetchScalarGridSpec(
            num_scalar_prefetch=1,
            grid=(2 * steps,),
            in_specs=[low_spec] * pieces + [high_spec] * pieces + right_specs + [row_spec] * len(bases),
            out_specs=row_spec,
        ),
        out_shape=jax.ShapeDtypeStruct((2 * half, width), out_type),
        compiler_params=pltpu.CompilerParams(dimension_semantics=("arbitrary",), vmem_limit_bytes=30 << 20),
        name="combined",
    )(side.reshape(1), *lows, *highs, *[r[0] for r in rights], *bases)


def body(tokens_in, cotangents, left_root, right_root):
    left, right = left_root[0], right_root[0, 0]
    width = right.shape[0]
    order = left.shape[0]
    experts = lax.axis_size(EXPERT)
    plane = lax.axis_size(PLANE)
    slots = tokens_in.shape[0] // experts
    z_size = lax.axis_size("z")
    side, sides = lax.axis_index("xl"), lax.axis_size("xl")

    sent = packed(cotangents, (2, 1, 3), sides, width)
    sent = [v.reshape(plane, slots, width) for v in sent]
    far, up, down = shift(sent[0], "z", 2), shift(sent[1], "z", 1), shift(sent[2], "z", -1)
    kept = packed(cotangents, (0,), sides, width)[0].reshape(plane, slots, width)

    tokens = exchange(tokens_in.reshape(experts, slots, order), EXPERT)
    low, high = left_applied(left, tokens.reshape(experts * slots, order))
    low_other, high_other = shift(low, "xl", 1), shift(high, "xl", 1)

    own = exchange(kept, PLANE)
    rest = exchange(jnp.stack([up, down, far], axis=1), PLANE)

    lows, highs = [], []
    for a, b in ((low, high), (low_other, high_other)):
        a_up, b_down = shift(a, "z", 1), shift(b, "z", -1)
        a_down, b_up = shift(a, "z", -1), shift(b, "z", 1)
        a_far, b_far = shift(a_up, "z", 1), shift(b_down, "z", -1)
        lows.append((a, a_up, a_down, a_far))
        highs.append((b, b_up, b_down, b_far))

    own = jnp.dot(own.reshape(-1, width), right, preferred_element_type=F32).astype(BF16)
    rest = jnp.dot(rest.reshape(-1, width), right, preferred_element_type=F32).astype(BF16)
    own = own.reshape(sides, experts * slots, width)
    rest = rest.reshape(sides, experts, z_size - 1, slots, width)
    most = combined(
        side,
        [v for row in lows for v in row[:3]],
        [v for row in highs for v in row[:3]],
        [r for o in (0, 1) for r in ((own, o, None), (rest, o, 0), (rest, o, 1))],
        None,
        F32,
    )
    update = combined(
        side, [row[3] for row in lows], [row[3] for row in highs], [(rest, 0, 2), (rest, 1, 2)], most, BF16
    )
    return update[None]


def solution(mesh):
    split = Mesh(mesh.devices.reshape(4, 2, 2, 4, 2), EXPERT + REPLICA)
    rows = P(EXPERT + REPLICA, None)
    placed = (rows, rows, P(EXPERT, None, None), P(EXPERT, REPLICA, None, None))

    return jax.shard_map(body, mesh=split, in_specs=placed, out_specs=P(EXPERT, None, REPLICA), check_vma=False)
```
